1024 devices in a mesh: prompt: 16 (over x, core), sample: 64 (over y, z).
Axes of the slice: x: 8, y: 8, z: 8, core: 2. Of those that a mesh axis runs over, the one named last changes fastest.
Arguments:
- latent: bfloat16 [1024, 576], P('prompt'), may hold values from -16 to 16
- queries: bfloat16 [4096, 128, 576], P('prompt', 'sample'), may hold values from -64 to 64
- cotangent: bfloat16 [4096, 128, 512], P('prompt', 'sample'), may hold values from -18 to 18
- suffix_out: bfloat16 [4096, 128, 512], P('prompt', 'sample'), may hold values from -6 to 6
- suffix_lse: bfloat16 [4096, 128], P('prompt', 'sample'), may hold values from 6 to 10
- rewards: float32 [16], replicated, may hold values from -5 to 5
- slot_sample: int32 [4096], P('prompt'), may hold values from 0 to 16, as said below
Outputs:
- query_grad: bfloat16 [4096, 128, 576], P('prompt', 'sample')
- latent_grad: float32 [1024, 576], P('prompt')
The draws below stay inside these ranges and needn't reach their ends.
Inputs may be any that keep to these rules, and one draw needn't show every extreme that they name: `slot_sample`: on every device the live slots come first and the others hold 16. Read over the devices in order, the live slots' completion numbers never fall, and every completion has a slot. Exactly 2048 slots are live in all, and some device has all 256 of its slots live.
All inputs are finite; a program needn't handle non-finite values.
Results may differ from the reference program's by a relative error of at most 0.006.
Values may be sent and summed in bfloat16 or wider, within the bound.
No kernel may reach another device: no remote copies, remote signals or barrier semaphores. Data moves between devices by JAX's collectives and lax.ppermute only.
A program may use at most 32 MiB of HBM per device.

```python
import math
import jax
import jax.numpy as jnp
from jax import lax

HEADS = 128
LATENT = 512
ROPE = 64
NOPE = 128
TOK_DEV = 256
PREFIX = 1024
SAMPLES = 16
TOKENS = 4096
N_PROMPT = 16


def prefix_and_queries(key):
    base_key = jax.random.fold_in(key, 101)
    width = LATENT + ROPE
    prefix_rows = jax.random.normal(jax.random.fold_in(base_key, 1), (PREFIX, width), jnp.float32)
    query_rows = 0.55 * jax.random.normal(jax.random.fold_in(base_key, 2), (TOKENS, HEADS, width), jnp.float32)
    return (jnp.clip(prefix_rows, -16.0, 16.0), jnp.clip(query_rows, -64.0, 64.0))


def draw_latent(key, part):
    return prefix_and_queries(key)[0].astype(jnp.bfloat16)


def draw_queries(key, part):
    return prefix_and_queries(key)[1].astype(jnp.bfloat16)


def draw_slot_sample(key, part):
    half_slots = TOK_DEV // 2
    pair_count = N_PROMPT // 2
    shuffled = jax.random.permutation(jax.random.fold_in(key, 11), N_PROMPT)
    shifts = jax.random.randint(jax.random.fold_in(key, 12), (pair_count,), -half_slots, half_slots + 1)
    shifts = shifts.at[0].set(half_slots)
    counts = jnp.zeros((N_PROMPT,), jnp.int32)
    counts = counts.at[shuffled[0::2]].set(half_slots + shifts)
    counts = counts.at[shuffled[1::2]].set(half_slots - shifts)
    live_total = N_PROMPT * half_slots
    boundaries = jnp.sort(jax.random.permutation(jax.random.fold_in(key, 13), live_total - 1)[:SAMPLES - 1] + 1)
    offsets = jnp.cumsum(counts) - counts
    slot_index = jnp.arange(TOK_DEV, dtype=jnp.int32)
    global_rank = offsets[:, None] + slot_index[None, :]
    sample_id = jnp.sum((boundaries[None, None, :] <= global_rank[:, :, None]).astype(jnp.int32), axis=2)
    marked = jnp.where(slot_index[None, :] < counts[:, None], sample_id, SAMPLES)
    return marked.reshape(TOKENS).astype(jnp.int32)


def level_of(key, dims, cuts, low, top_value):
    def one(position, parts):
        steps = jax.random.uniform(jax.random.fold_in(jax.random.fold_in(key, 6), position), (parts,), jnp.float32, low / len(cuts), top_value / len(cuts))
        return jnp.repeat(jnp.exp(steps), dims[position] // parts).reshape((-1,) + (1,) * (len(dims) - position - 1))

    gain = one(*cuts[0])
    for cut in cuts[1:]:
        gain = gain * one(*cut)
    return gain


def scatter_about(own_key, dims, spread, most, cuts=(), held_as=jnp.bfloat16):
    drawn = spread * jax.random.normal(own_key, dims, jnp.float32)
    if cuts:
        drawn = drawn * level_of(own_key, dims, cuts, -0.22, 0.18)
    return jnp.clip(drawn, -most, most).astype(held_as)


def setup_inputs(seed: int = 0) -> dict:
    key_list = jax.random.split(jax.random.key(seed), 8)
    return {
        "latent": draw_latent(jax.random.fold_in(key_list[7], 71), 0),
        "queries": draw_queries(jax.random.fold_in(key_list[7], 71), 0),
        "cotangent": scatter_about(key_list[2], (TOKENS, HEADS, LATENT), 3.0, 18.0, ((0, 16), (1, 64))),
        "suffix_out": scatter_about(key_list[3], (TOKENS, HEADS, LATENT), 1.0, 6.0, ((0, 16), (1, 64))),
        "suffix_lse": jnp.clip(6.0 + 4.0 * jax.random.uniform(key_list[4], (TOKENS, HEADS), jnp.float32) ** level_of(key_list[4], (TOKENS, HEADS), ((0, 16), (1, 64)), -0.2, 0.2), 6.0, 10.0).astype(jnp.bfloat16),
        "rewards": scatter_about(key_list[5], (SAMPLES,), 1.0, 5.0, (), jnp.float32),
        "slot_sample": draw_slot_sample(jax.random.fold_in(key_list[7], 71), 0),
    }


def softmax_scale():
    return (0.1 * math.log(40.0) + 1.0) ** 2 / math.sqrt(NOPE + ROPE)

def advantages(rewards, slot_sample):
    centred = rewards - jnp.mean(rewards)
    advantage_table = jnp.concatenate([centred, jnp.zeros((1,), jnp.float32)])
    sample_ids = jnp.arange(advantage_table.shape[0], dtype=jnp.int32)
    return lax.optimization_barrier(jnp.sum(jnp.where(slot_sample[:, None] == sample_ids[None, :], advantage_table[None, :], 0.0), axis=1))

def reference(latent, queries, cotangent, suffix_out, suffix_lse, rewards, slot_sample):
    factor = softmax_scale()
    weight = advantages(rewards, slot_sample)
    values = latent[:, :LATENT]

    def one_head(running, head_index):
        head_query = lax.dynamic_index_in_dim(queries, head_index, 1, keepdims=False)
        head_cot = lax.dynamic_index_in_dim(cotangent, head_index, 1, keepdims=False)
        head_suffix = lax.dynamic_index_in_dim(suffix_out, head_index, 1, keepdims=False)
        head_lse = lax.dynamic_index_in_dim(suffix_lse, head_index, 1, keepdims=False).astype(jnp.float32)
        scores = factor * jnp.dot(head_query, latent.T, preferred_element_type=jnp.float32)
        row_max = lax.optimization_barrier(jnp.max(scores, axis=1))
        prefix_lse = row_max + jnp.log(lax.optimization_barrier(jnp.sum(jnp.exp(scores - row_max[:, None]), axis=1)))
        joint_max = jnp.maximum(prefix_lse, head_lse)
        total_lse = joint_max + jnp.log(jnp.exp(prefix_lse - joint_max) + jnp.exp(head_lse - joint_max))
        probability = jnp.exp(scores - total_lse[:, None])
        scaled = (weight[:, None] * head_cot.astype(jnp.float32)).astype(jnp.bfloat16)
        prob_grad = jnp.dot(scaled, values.T, preferred_element_type=jnp.float32)
        suffix_dot = lax.optimization_barrier(jnp.sum(scaled.astype(jnp.float32) * head_suffix.astype(jnp.float32), axis=1))
        row_delta = lax.optimization_barrier(jnp.sum(probability * prob_grad, axis=1)) + jnp.exp(head_lse - total_lse) * suffix_dot
        score_grad = (factor * probability * (prob_grad - row_delta[:, None])).astype(jnp.bfloat16)
        head_grad = jnp.dot(score_grad, latent, preferred_element_type=jnp.float32).astype(jnp.bfloat16)
        key_term = jnp.dot(score_grad.T, head_query, preferred_element_type=jnp.float32)
        value_term = jnp.dot(probability.astype(jnp.bfloat16).T, scaled, preferred_element_type=jnp.float32)
        latent_term = key_term + jnp.pad(value_term, ((0, 0), (0, ROPE)))
        return (running + latent_term, head_grad)
    start_sum = jnp.zeros((PREFIX, LATENT + ROPE), jnp.float32)
    running, head_grads = lax.scan(one_head, start_sum, jnp.arange(HEADS, dtype=jnp.int32))
    return (jnp.transpose(head_grads, (1, 0, 2)), running)
```

```python
import math

import jax
import jax.numpy as jnp
from jax import lax
from jax.sharding import Mesh, PartitionSpec as P

ROPE = 64
NOPE = 128


def softmax_scale():
    return (0.1 * math.log(40.0) + 1.0) ** 2 / math.sqrt(NOPE + ROPE)


def to_partner(value):
    return lax.ppermute(value, "core", [(0, 1), (1, 0)])


def exchanged(pieces, axes):
    return lax.all_to_all(pieces, axes, 0, 0, tiled=True)


def attend(queries, scaled, suffix_dot, suffix_lse, keys, factor):
    value_width = scaled.shape[-1]
    scores = factor * jnp.einsum("thd,pd->htp", queries, keys, preferred_element_type=jnp.float32)
    row_max = jnp.max(scores, axis=2)
    prefix_lse = row_max + jnp.log(jnp.sum(jnp.exp(scores - row_max[..., None]), axis=2))
    tail_lse = suffix_lse.astype(jnp.float32).T
    joint_max = jnp.maximum(prefix_lse, tail_lse)
    total_lse = joint_max + jnp.log(jnp.exp(prefix_lse - joint_max) + jnp.exp(tail_lse - joint_max))
    probability = jnp.exp(scores - total_lse[..., None])
    prob_grad = jnp.einsum(
        "thd,pd->htp", scaled, keys[:, :value_width], preferred_element_type=jnp.float32
    )
    row_delta = (
        jnp.sum(probability * prob_grad, axis=2) + jnp.exp(tail_lse - total_lse) * suffix_dot.T
    )
    score_grad = (factor * probability * (prob_grad - row_delta[..., None])).astype(jnp.bfloat16)
    weights = probability.astype(jnp.bfloat16)

    def query_grad():
        return jnp.einsum(
            "htp,pd->thd", score_grad, keys, preferred_element_type=jnp.float32
        ).astype(jnp.bfloat16)

    def key_grad(first, count):
        rows = slice(first, first + count)
        key_term = jnp.einsum(
            "htp,thd->pd", score_grad[..., rows], queries, preferred_element_type=jnp.float32
        )
        value_term = jnp.einsum(
            "htp,thd->pd", weights[..., rows], scaled, preferred_element_type=jnp.float32
        )
        return key_term + jnp.pad(value_term, ((0, 0), (0, key_term.shape[1] - value_width)))

    return query_grad, key_grad


def on_device(latent, queries, cotangent, suffix_out, suffix_lse, rewards, slot_sample):
    factor = softmax_scale()
    chips = lax.axis_size("x")
    ys, zs = lax.axis_size("y"), lax.axis_size("z")
    rows, width = latent.shape
    half = chips * rows

    mine = exchanged(jnp.broadcast_to(latent[None], (chips, rows, width)), "x").reshape(half, width)
    keys = jnp.concatenate([mine, to_partner(mine)], axis=0)

    centred = rewards - jnp.mean(rewards)
    advantage_table = jnp.concatenate([centred, jnp.zeros((1,), jnp.float32)])
    sample_ids = jnp.arange(advantage_table.shape[0], dtype=jnp.int32)
    weight = jnp.sum(
        jnp.where(slot_sample[:, None] == sample_ids[None, :], advantage_table[None, :], 0.0),
        axis=1,
    )
    scaled = (weight[:, None, None] * cotangent.astype(jnp.float32)).astype(jnp.bfloat16)
    suffix_dot = jnp.sum(scaled.astype(jnp.float32) * suffix_out.astype(jnp.float32), axis=2)

    query_grad, key_grad = attend(queries, scaled, suffix_dot, suffix_lse, keys, factor)
    received = to_partner(key_grad(half, half))
    on_chip = (key_grad(0, half) + received).astype(jnp.bfloat16)

    pieces = exchanged(on_chip.reshape(chips * ys, rows // ys, width), ("x", "y"))
    part = jnp.sum(pieces.astype(jnp.float32), axis=0).astype(jnp.bfloat16)
    copies = exchanged(jnp.broadcast_to(part[None], (ys * zs, *part.shape)), ("y", "z"))
    copies = copies.reshape(ys, zs, rows // ys, width).astype(jnp.float32)
    latent_grad = jnp.sum(copies, axis=1).reshape(rows, width)
    return query_grad(), latent_grad


def solution(mesh):
    prompt, sample = mesh.devices.shape
    side = math.isqrt(sample)
    grid = Mesh(
        mesh.devices.reshape(prompt // 2, 2, side, sample // side), ("x", "core", "y", "z")
    )
    slots, heads = ("x", "core"), ("y", "z")
    in_specs = (
        P(slots, None),
        P(slots, heads, None),
        P(slots, heads, None),
        P(slots, heads, None),
        P(slots, heads),
        P(),
        P(slots),
    )
    out_specs = (P(slots, heads, None), P(slots, None))
    return jax.shard_map(
        on_device, mesh=grid, in_specs=in_specs, out_specs=out_specs, check_vma=False
    )
```

```python
import math

import jax
import jax.numpy as jnp
from jax import lax
from jax.experimental import pallas as pl
from jax.experimental.pallas import tpu as pltpu
from jax.sharding import Mesh, PartitionSpec as P

ROPE = 64
NOPE = 128
VMEM_BYTES = 20 * 1024 * 1024


def softmax_scale():
    return (0.1 * math.log(40.0) + 1.0) ** 2 / math.sqrt(NOPE + ROPE)


def to_partner(value):
    return lax.ppermute(value, "core", [(0, 1), (1, 0)])


def exchanged(pieces, axes):
    return lax.all_to_all(pieces, axes, 0, 0, tiled=True)


def dot(a, b, dims=((1,), (0,))):
    return lax.dot_general(a, b, (dims, ((), ())), preferred_element_type=jnp.float32)


def key_grad(score_grad, weights, queries, scaled, out_ref):
    value_width = scaled.shape[-1]
    key_term = dot(score_grad, queries)
    owners, rows, _ = out_ref.shape
    value_term = key_term[:, :value_width] + dot(weights, scaled)
    out_ref[:, :, :value_width] = value_term.reshape(owners, rows, value_width)
    out_ref[:, :, value_width:] = key_term[:, value_width:].reshape(owners, rows, -1)


def joined(keys):
    return keys[...].reshape(-1, keys.shape[-1])


def scores_of(keys, queries_t, scaled_t):
    return (
        softmax_scale() * dot(keys, queries_t),
        dot(keys[:, : scaled_t.shape[0]], scaled_t),
    )


def scores_kernel(mine, queries_t, scaled_t, scores, prob_grad):
    heads, _, slots = queries_t.shape
    keys = joined(mine)
    for h in range(heads):
        columns = pl.ds(h * slots, slots)
        scores[:, columns], prob_grad[:, columns] = scores_of(keys, queries_t[h], scaled_t[h])


def softmax_kernel(
    other, my_scores, my_prob_grad, queries_t, scaled_t, queries, scaled, suffix_dot, suffix_lse,
    sent_grad, score_grad, weights,
):
    factor = softmax_scale()
    heads, _, slots = queries_t.shape
    half = other.shape[0] * other.shape[1]
    keys = joined(other)
    other_weights = []
    for h in range(heads):
        columns = pl.ds(h * slots, slots)
        other_scores, other_prob_grad = scores_of(keys, queries_t[h], scaled_t[h])
        scores = (my_scores[:, columns], other_scores)
        prob_grad = (my_prob_grad[:, columns], other_prob_grad)
        row_max = jnp.maximum(*[jnp.max(s, axis=0, keepdims=True) for s in scores])
        powers = [jnp.exp(s - row_max) for s in scores]
        total = sum(jnp.sum(p, axis=0, keepdims=True) for p in powers)
        prefix_lse = row_max + jnp.log(total)
        tail_lse = suffix_lse[h : h + 1, :]
        joint_max = jnp.maximum(prefix_lse, tail_lse)
        total_lse = joint_max + jnp.log(
            jnp.exp(prefix_lse - joint_max) + jnp.exp(tail_lse - joint_max)
        )
        share = jnp.exp(row_max - total_lse)
        prefix_dot = sum(
            jnp.sum(p * g, axis=0, keepdims=True) for p, g in zip(powers, prob_grad)
        )
        row_delta = share * prefix_dot + jnp.exp(tail_lse - total_lse) * suffix_dot[h : h + 1, :]
        for i in range(2):
            probability = powers[i] * share
            grad = factor * probability * (prob_grad[i] - row_delta)
            score_grad[pl.ds(i * half, half), columns] = grad.astype(jnp.bfloat16)
            if i == 0:
                weights[:, columns] = probability.astype(jnp.bfloat16)
            else:
                other_weights.append(probability.astype(jnp.bfloat16))
    key_grad(
        score_grad[pl.ds(half, half), :],
        jnp.concatenate(other_weights, axis=1),
        queries[...],
        scaled[...],
        sent_grad,
    )


def rest_kernel(
    mine, other, queries, scaled, score_grad, weights, kept_grad, query_grad_t
):
    half = mine.shape[0] * mine.shape[1]
    heads, _, slots = query_grad_t.shape
    key_grad(score_grad[:half, :], weights[...], queries[...], scaled[...], kept_grad)
    rows = ((0,), (0,))
    query_grad = dot(joined(mine), score_grad[:half, :], rows)
    query_grad += dot(joined(other), score_grad[pl.ds(half, half), :], rows)
    for h in range(heads):
        query_grad_t[h] = query_grad[:, h * slots : (h + 1) * slots].astype(jnp.bfloat16)


def call(kernel, name, outs, *args):
    return pl.pallas_call(
        kernel,
        out_shape=outs,
        name=name,
        compiler_params=pltpu.CompilerParams(vmem_limit_bytes=VMEM_BYTES),
    )(*args)


def prepared(queries, cotangent, suffix_out, suffix_lse, rewards, slot_sample):
    slots, heads, width = queries.shape
    centred = rewards - jnp.mean(rewards)
    advantage_table = jnp.concatenate([centred, jnp.zeros((1,), jnp.float32)])
    sample_ids = jnp.arange(advantage_table.shape[0], dtype=jnp.int32)
    weight = jnp.sum(
        jnp.where(slot_sample[:, None] == sample_ids[None, :], advantage_table[None, :], 0.0),
        axis=1,
    )
    scaled = (weight[:, None, None] * cotangent.astype(jnp.float32)).astype(jnp.bfloat16)
    suffix_dot = jnp.sum(scaled.astype(jnp.float32) * suffix_out.astype(jnp.float32), axis=2)
    return (
        jnp.transpose(queries, (1, 2, 0)),
        jnp.transpose(scaled, (1, 2, 0)),
        jnp.transpose(queries, (1, 0, 2)).reshape(heads * slots, width),
        jnp.transpose(scaled, (1, 0, 2)).reshape(heads * slots, -1),
        suffix_dot.T,
        suffix_lse.astype(jnp.float32).T,
    )


def scores_part(mine, ready):
    queries_t, scaled_t = ready[:2]
    heads, _, slots = queries_t.shape
    out = jax.ShapeDtypeStruct((mine.shape[0] * mine.shape[1], heads * slots), jnp.float32)
    return call(scores_kernel, "scores", (out, out), mine, queries_t, scaled_t)


def softmax_part(other, my_scores, ready):
    queries_t, scaled_t, queries_r, scaled_r, suffix_dot, tail_lse = ready
    heads, _, slots = queries_t.shape
    half = other.shape[0] * other.shape[1]
    return call(
        softmax_kernel,
        "softmax",
        (
            jax.ShapeDtypeStruct(other.shape, jnp.float32),
            jax.ShapeDtypeStruct((2 * half, heads * slots), jnp.bfloat16),
            jax.ShapeDtypeStruct((half, heads * slots), jnp.bfloat16),
        ),
        other, *my_scores, queries_t, scaled_t, queries_r, scaled_r, suffix_dot, tail_lse,
    )


def rest_part(mine, other, ready, score_grad, weights):
    queries_t, _, queries_r, scaled_r, _, _ = ready
    return call(
        rest_kernel,
        "rest",
        (
            jax.ShapeDtypeStruct(mine.shape, jnp.float32),
            jax.ShapeDtypeStruct(queries_t.shape, jnp.bfloat16),
        ),
        mine, other, queries_r, scaled_r, score_grad, weights,
    )


def on_device(latent, queries, cotangent, suffix_out, suffix_lse, rewards, slot_sample):
    chips = lax.axis_size("x")
    ys, zs = lax.axis_size("y"), lax.axis_size("z")
    rows, width = latent.shape

    mine = exchanged(jnp.broadcast_to(latent[None], (chips, rows, width)), "x")
    ready = prepared(queries, cotangent, suffix_out, suffix_lse, rewards, slot_sample)
    mine, ready = lax.optimization_barrier((mine, ready))
    other = to_partner(mine)
    sent_grad, score_grad, weights = softmax_part(other, scores_part(mine, ready), ready)
    received = to_partner(sent_grad)
    kept_grad, query_grad_t = rest_part(mine, other, ready, score_grad, weights)
    on_chip = (kept_grad + received).astype(jnp.bfloat16)

    pieces = exchanged(on_chip.reshape(chips * ys, rows // ys, width), ("x", "y"))
    part = jnp.sum(pieces.astype(jnp.float32), axis=0).astype(jnp.bfloat16)
    copies = exchanged(jnp.broadcast_to(part[None], (ys * zs, *part.shape)), ("y", "z"))
    copies = copies.reshape(ys, zs, rows // ys, width).astype(jnp.float32)
    latent_grad = jnp.sum(copies, axis=1).reshape(rows, width)
    return jnp.transpose(query_grad_t, (2, 0, 1)), latent_grad


def solution(mesh):
    prompt, sample = mesh.devices.shape
    side = math.isqrt(sample)
    grid = Mesh(
        mesh.devices.reshape(prompt // 2, 2, side, sample // side), ("x", "core", "y", "z")
    )
    slots, heads = ("x", "core"), ("y", "z")
    in_specs = (
        P(slots, None),
        P(slots, heads, None),
        P(slots, heads, None),
        P(slots, heads, None),
        P(slots, heads),
        P(),
        P(slots),
    )
    out_specs = (P(slots, heads, None), P(slots, None))
    return jax.shard_map(
        on_device, mesh=grid, in_specs=in_specs, out_specs=out_specs, check_vma=False
    )
```
